128 devices in a mesh: pipe: 4 (over y_hi, core), exp: 16 (over x, z), pair: 2 (over y_lo).
Axes of the slice: x: 4, y: 4 (y_hi: 2, y_lo: 2; y = y_hi * 2 + y_lo), z: 4, core: 2. Of those that a mesh axis runs over, the one named last changes fastest.
Arguments:
- hidden_in: bfloat16 [4, 1024, 2048], P(None, ('exp', 'pair')), may hold values from -6 to 6
- routes: int32 [4, 4, 1024, 8], P('pipe', None, ('exp', 'pair')), may hold values from 0 to 63, all different within a row; in each aligned block of 32 rows (0 to 31, 32 to 63, ..., all dimensions but the last counted through in order) at most 6 rows name the same one
- gate_probs: float32 [4, 4, 1024, 8], P('pipe', None, ('exp', 'pair')), may hold values from 0.02 to 1
- norm_gain: float32 [4, 2048], P('pipe'), may hold values from 0.1 to 1.9
- w_gate: bfloat16 [4, 64, 2048, 768], P('pipe', ('exp', 'pair')), may hold values from -0.125 to 0.125
- w_up: bfloat16 [4, 64, 2048, 768], P('pipe', ('exp', 'pair')), may hold values from -0.125 to 0.125
- w_down: bfloat16 [4, 64, 768, 2048], P('pipe', ('exp', 'pair')), may hold values from -0.21875 to 0.21875
Outputs:
- layer_outputs: bfloat16 [4, 4, 1024, 2048], P('pipe', None, ('exp', 'pair'))
The draws below stay inside these ranges and needn't reach their ends.
Inputs may be any that keep to these rules, and one draw needn't show every extreme that they name: `routes`: within each layer and micro-batch, the 32 tokens of one device (aligned blocks) name no expert more than 6 times in all, and each token names 8 different experts.
All inputs are finite; a program needn't handle non-finite values.
Results may differ from the reference program's by a relative error of at most 0.01.
Values may be sent and summed in bfloat16 or wider, within the bound.
A program may use at most 64 MiB of HBM per device.

```python
import math
import jax
import jax.numpy as jnp
import numpy as np
from jax import lax

D = 2048
FF = 768
TOPK = 8
MB = 4
TOK_DEV = 32
EXPERTS = 64
LAYERS = 4
TOKENS = 1024
CAP = 6


def block_scale(rng, shape, shards, least, largest):
    def one(position, parts):
        steps = jax.random.uniform(jax.random.fold_in(jax.random.fold_in(rng, 6), position), (parts,), jnp.float32, least / len(shards), largest / len(shards))
        return jnp.repeat(jnp.exp(steps), shape[position] // parts).reshape((-1,) + (1,) * (len(shape) - position - 1))

    loudness = one(*shards[0])
    for cut in shards[1:]:
        loudness = loudness * one(*cut)
    return loudness


def routed_block(rng, own, number, rows, number_of, top, bound, skew):
    order = jax.random.permutation(rng, number_of)
    packed, common = shares(number_of, rows * top, bound, skew, True), shares(number_of, rows * top, bound, skew, False)
    places = jnp.arange(number_of)

    def named(sizes, rotation):
        used = int((sizes > 0).sum())
        fixed = max(1, used // 4)
        shifted = fixed + (places - fixed + rotation * (used - fixed)) % max(1, number_of - fixed)
        return jnp.zeros((number_of,), jnp.int32).at[order[jnp.where(places < fixed, places, shifted)]].set(jnp.asarray(sizes, jnp.int32))

    sizes = jnp.where(number % 4 == 0, named(packed, number // 4), named(common, number - number // 4 - 1))
    mixed = jax.random.permutation(jax.random.fold_in(own, 3), number_of)
    donor, taker = mixed[0:number_of // 2 * 2:2], mixed[1:number_of // 2 * 2:2]
    margin = jnp.minimum(sizes[donor] - 1, bound - sizes[taker]) // 2
    margin = jnp.where((donor == order[0]) | (taker == order[0]) | (sizes[taker] == 0), 0, jnp.maximum(margin, 0))
    shifted = jax.random.randint(jax.random.fold_in(own, 4), (number_of // 2,), 0, 1 << 20) % (margin + 1)
    sizes = sizes.at[donor].add(-shifted).at[taker].add(shifted)
    labels = jnp.searchsorted(jnp.cumsum(sizes), jnp.arange(rows * top), side="right").astype(jnp.int32)
    grid = labels.reshape(top, rows).T
    grid = grid[jax.random.permutation(jax.random.fold_in(own, 1), rows)]
    rotation = jax.random.randint(jax.random.fold_in(own, 2), (rows, 1), 0, top)
    return jnp.take_along_axis(grid, (jnp.arange(top)[None, :] + rotation) % top, axis=1)


def shares(number_of, total, most, skew, full):
    loads = [(1 << 20) // math.isqrt(grade ** skew) + 1 for grade in range(1, number_of + 1)]
    largest = most if full else min(most, max(-(-total // number_of), total * loads[0] // sum(loads)))
    least = 1 if total - largest >= number_of - 1 else 0
    counts, surplus = [largest] + [least] * (number_of - 1), total - largest - least * (number_of - 1)
    while surplus > 0:
        candidates = [i for i in range(1, number_of) if counts[i] < largest] or [i for i in range(1, number_of) if counts[i] < most]
        mass, remaining = sum([loads[i] for i in candidates]), surplus
        for i in candidates:
            addition = min(most - counts[i], max(1, remaining * loads[i] // mass), surplus)
            counts[i] = counts[i] + addition
            surplus = surplus - addition
    return np.array(counts)


def normal_values(own_key, dims, width, most, shards=(), held_as=jnp.bfloat16):
    drawn = jax.random.normal(own_key, dims, jnp.float32) * width
    if len(shards) > 0:
        drawn = block_scale(own_key, dims, shards, -0.22, 0.18) * drawn
    return jnp.clip(drawn, min=-most, max=most).astype(held_as)


def setup_inputs(seed: int = 0) -> dict:
    key_of = jax.random.split(jax.random.key(seed), 8)
    hidden_in = normal_values(key_of[0], (MB, TOKENS, D), 1.0, 6.0, ((1, 32),))
    routes_keys = jax.random.split(jax.random.fold_in(key_of[1], 1), LAYERS * MB * TOKENS // TOK_DEV)
    routes_turns = jax.random.permutation(jax.random.fold_in(key_of[1], 3), LAYERS * MB * TOKENS // TOK_DEV)
    routes = jax.vmap(lambda own, number: routed_block(jax.random.fold_in(key_of[1], 2), own, number, TOK_DEV, EXPERTS, TOPK, CAP, 2))(routes_keys, routes_turns).reshape((LAYERS, MB, TOKENS, TOPK))
    gate_probs = jnp.clip(jnp.exp(math.log(1.0) - 3.912023 * jax.random.uniform(key_of[2], (LAYERS, MB, TOKENS, TOPK), jnp.float32) ** block_scale(key_of[2], (LAYERS, MB, TOKENS, TOPK), ((0, 4), (2, 32)), -0.2, 0.2)), 0.02, 1.0)
    norm_gain = jnp.clip(1.0 + 0.18 * jax.random.normal(key_of[3], (LAYERS, D), jnp.float32), 0.1, 1.9)
    w_gate = normal_values(key_of[4], (LAYERS, EXPERTS, D, FF), D ** -0.5, 0.125, ((0, 4), (1, 32)))
    w_up = normal_values(key_of[5], (LAYERS, EXPERTS, D, FF), D ** -0.5, 0.125, ((0, 4), (1, 32)))
    w_down = normal_values(key_of[6], (LAYERS, EXPERTS, FF, D), FF ** -0.5, 0.21875, ((0, 4), (1, 32)))
    return {"hidden_in": hidden_in, "routes": routes, "gate_probs": gate_probs, "norm_gain": norm_gain, "w_gate": w_gate, "w_up": w_up, "w_down": w_down}


EPS = 1e-06

def slots_of(block_routes):
    expert_ids = jnp.arange(EXPERTS, dtype=jnp.int32)
    onehot = (block_routes[:, None] == expert_ids[None, :]).astype(jnp.int32)
    before = jnp.cumsum(onehot, axis=0) - onehot
    return lax.optimization_barrier(jnp.sum(before * onehot, axis=1)).astype(jnp.int32)

def moe_layer(state, chosen, probs, gain, wgate, wupper, wdown):
    floated = state.astype(jnp.float32)
    scale = lax.rsqrt(lax.optimization_barrier(jnp.mean(floated * floated, axis=-1, keepdims=True)) + EPS)
    normed = (floated * scale * gain.astype(jnp.float32)).astype(jnp.bfloat16)
    blocks = TOKENS // TOK_DEV
    flat_routes = chosen.reshape(blocks, TOK_DEV * TOPK).astype(jnp.int32)
    slots = jax.vmap(slots_of)(flat_routes)
    columns = (slots + CAP * jnp.arange(blocks, dtype=jnp.int32)[:, None]).reshape(-1)
    rows_ids = flat_routes.reshape(-1)
    buffer = jnp.zeros((EXPERTS, blocks * CAP, D), jnp.bfloat16)
    buffer = buffer.at[rows_ids, columns].set(jnp.repeat(normed, TOPK, axis=0))

    def one_expert(items):
        inputs, gate_w, up_w, down_w = items
        gate = jnp.dot(inputs, gate_w, preferred_element_type=jnp.float32)
        upward = jnp.dot(inputs, up_w, preferred_element_type=jnp.float32)
        hidden = (jax.nn.silu(gate) * upward).astype(jnp.bfloat16)
        return jnp.dot(hidden, down_w, preferred_element_type=jnp.float32).astype(jnp.bfloat16)
    produced = lax.map(one_expert, (buffer, wgate, wupper, wdown))
    picked = produced[rows_ids, columns].reshape(TOKENS, TOPK, D).astype(jnp.float32)
    probs32 = probs.astype(jnp.float32)
    weights = probs32 / lax.optimization_barrier(jnp.sum(probs32, axis=-1, keepdims=True))
    mixed = jnp.einsum('tk,tkd->td', weights, picked)
    return (floated + mixed).astype(jnp.bfloat16)

def reference(hidden_in, routes, gate_probs, norm_gain, w_gate, w_up, w_down):
    current = hidden_in
    outputs = []
    for layer in range(LAYERS):

        def per_batch(items):
            state, chosen, probs = items
            return moe_layer(state, chosen, probs, norm_gain[layer], w_gate[layer], w_up[layer], w_down[layer])
        current = lax.map(per_batch, (current, routes[layer], gate_probs[layer]))
        outputs.append(current)
    return jnp.stack(outputs, axis=0)
```

```python
import functools

import jax
import jax.numpy as jnp
from jax import lax
from jax.experimental import pallas as pl
from jax.experimental.pallas import tpu as pltpu
from jax.sharding import PartitionSpec as P

EPS = 1e-06
MESH = pl.DeviceIdType.MESH
F32 = jnp.float32
BF16 = jnp.bfloat16
VMEM_LIMIT = 63 * 1024 * 1024
SLOTS = 6
SIDE = 4
QUARTERS = 4
CHUNKS = 2
LANES = 128
UNITS = 8


def fdiv(value, n):
    return jnp.floor((value + 0.5) * (1.0 / n))


def iota(shape, axis):
    return lax.broadcasted_iota(jnp.int32, shape, axis).astype(F32)


def dot(a, b):
    return jnp.dot(a, b, preferred_element_type=F32)


def dot_nt(a, b):
    return lax.dot_general(a, b, (((1,), (1,)), ((), ())), preferred_element_type=F32)


def relay_kernel(
    stages,
    zs,
    ys,
    hidden_ref,
    routes_ref,
    probs_ref,
    gain_ref,
    wgate_ref,
    wup_ref,
    wdown_ref,
    out_ref,
    wg,
    wu,
    wd,
    hbuf,
    obuf,
    xq,
    sendbuf,
    recvbuf,
    backbuf,
    homebuf,
    xe,
    acc,
    hid,
    stack,
    sel,
    pick_g,
    pick_s,
    gath,
    comb,
    unpack,
    repack,
    w_sem,
    h_sem,
    hs_sem,
    o_sem,
    a_sem,
    ar_sem,
    b_sem,
    br_sem,
):
    micro, rows, width = hbuf.shape
    locals_, _, ff = wg.shape
    groups = zs * ys
    block = QUARTERS * locals_ * SLOTS
    total = groups * block
    half = locals_ * SLOTS
    cw = width // CHUNKS
    qw = cw // QUARTERS
    unit = UNITS * block
    units = groups // UNITS
    per = UNITS * SLOTS
    erows = groups * SLOTS

    stage = lax.axis_index("pipe")
    e_idx = lax.axis_index("exp")
    y = lax.axis_index("pair")
    me = e_idx * ys + y
    cx = lax.div(e_idx, SIDE)
    cz = lax.rem(e_idx, SIDE)

    def ring(d):
        return min(d, SIDE - d)

    offsets = [
        (dx, dz, dy)
        for dx in range(zs // SIDE)
        for dz in range(SIDE)
        for dy in range(ys)
        if dx or dz or dy
    ]
    offsets.sort(key=lambda o: -(ring(o[0]) + ring(o[1]) + o[2]))

    def peer(offset):
        dx, dz, dy = offset
        px = lax.rem(cx + dx, zs // SIDE)
        pz = lax.rem(cz + dz, SIDE)
        return px * SIDE + pz, lax.rem(y + dy, ys)

    loads = []
    for j in range(locals_):
        loads.append(
            (
                pltpu.make_async_copy(wgate_ref.at[0, j], wg.at[j], w_sem.at[3 * j]),
                pltpu.make_async_copy(wup_ref.at[0, j], wu.at[j], w_sem.at[3 * j + 1]),
                pltpu.make_async_copy(wdown_ref.at[0, j], wd.at[j], w_sem.at[3 * j + 2]),
            )
        )

    def from_input(m):
        return pltpu.make_async_copy(hidden_ref.at[m], hbuf.at[m], h_sem.at[m])

    @pl.when(stage == 0)
    def _():
        for m in range(micro):
            from_input(m).start()

    for j in range(locals_):
        loads[j][0].start()
        loads[j][1].start()
    for j in range(locals_):
        loads[j][2].start()

    barrier = pltpu.get_barrier_semaphore()
    for offset in offsets:
        pe, py = peer(offset)
        pl.semaphore_signal(barrier, inc=1, device_id={"exp": pe, "pair": py}, device_id_type=MESH)

    @pl.when(stage > 0)
    def _():
        pl.semaphore_signal(barrier, inc=1, device_id={"pipe": stage - 1}, device_id_type=MESH)

    @pl.when(stage < stages - 1)
    def _():
        pl.semaphore_signal(barrier, inc=1, device_id={"pipe": stage + 1}, device_id_type=MESH)

    def row_parts(index):
        d = fdiv(index, block)
        r = index - block * d
        q = fdiv(r, half)
        t = r - half * q
        j = fdiv(t, SLOTS)
        return d, q, j, t - SLOTS * j

    for u in range(units):
        here = pl.ds(u * unit, unit)
        d, q, j, s = row_parts(iota((unit, LANES), 0) + u * unit)
        lane = iota((unit, LANES), 1)
        sel[here] = jnp.where(lane == locals_ * d + j, 1.0, 0.0).astype(BF16)
        pick_g[here] = jnp.where(fdiv(lane, rows) == q, s + 1.0, -1.0)
        d, q, j, s = row_parts(iota((QUARTERS * rows, unit), 1) + u * unit)
        at = iota((QUARTERS * rows, unit), 0)
        pick_s[:, u * unit : (u + 1) * unit] = jnp.where(fdiv(at, rows) == q, s + 1.0, -1.0)
    d, q, j, s = row_parts(iota((unit, unit), 1))
    spread = (q * locals_ + j) * per + d * SLOTS + s
    unpack[...] = jnp.where(iota((unit, unit), 0) == spread, 1.0, 0.0).astype(BF16)
    d, q, j, s = row_parts(iota((unit, unit), 0))
    spread = (q * locals_ + j) * per + d * SLOTS + s
    repack[...] = jnp.where(iota((unit, unit), 1) == spread, 1.0, 0.0).astype(BF16)

    linked = (stage > 0).astype(jnp.int32) + (stage < stages - 1).astype(jnp.int32)
    pl.semaphore_wait(barrier, len(offsets) + linked)

    def part_of(at):
        return pl.ds(pl.multiple_of(at * block, block), block)

    def out_copy_of(m, c, at, pe, py):
        return pltpu.make_async_remote_copy(
            src_ref=sendbuf.at[m, c, part_of(at)],
            dst_ref=recvbuf.at[m, c, part_of(me)],
            send_sem=a_sem.at[m, c, at],
            recv_sem=ar_sem.at[m, c, me],
            device_id={"exp": pe, "pair": py},
            device_id_type=MESH,
        )

    def in_copy_of(m, c, at, pe, py):
        return pltpu.make_async_remote_copy(
            src_ref=sendbuf.at[m, c, part_of(at)],
            dst_ref=recvbuf.at[m, c, part_of(at)],
            send_sem=a_sem.at[m, c, at],
            recv_sem=ar_sem.at[m, c, at],
            device_id={"exp": pe, "pair": py},
            device_id_type=MESH,
        )

    def back_copy_of(m, c, at, pe, py):
        return pltpu.make_async_remote_copy(
            src_ref=backbuf.at[m, c, part_of(at)],
            dst_ref=homebuf.at[m, c, part_of(me)],
            send_sem=b_sem.at[m, c, at],
            recv_sem=br_sem.at[m, c, me],
            device_id={"exp": pe, "pair": py},
            device_id_type=MESH,
        )

    def home_copy_of(m, c, at, pe, py):
        return pltpu.make_async_remote_copy(
            src_ref=backbuf.at[m, c, part_of(at)],
            dst_ref=homebuf.at[m, c, part_of(at)],
            send_sem=b_sem.at[m, c, at],
            recv_sem=br_sem.at[m, c, at],
            device_id={"exp": pe, "pair": py},
            device_id_type=MESH,
        )

    def hand_copy(m):
        return pltpu.make_async_remote_copy(
            src_ref=obuf.at[m],
            dst_ref=hbuf.at[m],
            send_sem=hs_sem.at[m],
            recv_sem=h_sem.at[m],
            device_id={"pipe": stage + 1},
            device_id_type=MESH,
        )

    def out_copy(m):
        return pltpu.make_async_copy(obuf.at[m], out_ref.at[0, m], o_sem.at[m])

    earlier = (iota((rows, rows), 0) >= iota((rows, rows), 1)).astype(F32).astype(BF16)

    def dispatch(m):
        chosen = routes_ref[0, m]
        probs = probs_ref[0, m]
        normal = probs / jnp.sum(probs, axis=-1, keepdims=True)
        lane = lax.broadcasted_iota(jnp.int32, (rows, LANES), 1)
        mask = jnp.zeros((rows, LANES), F32)
        weight = jnp.zeros((rows, LANES), F32)
        for k in range(chosen.shape[1]):
            hit = lane == chosen[:, k : k + 1]
            mask = mask + jnp.where(hit, 1.0, 0.0)
            weight = weight + jnp.where(hit, normal[:, k : k + 1], 0.0)
        code = (mask * dot(earlier, mask.astype(BF16))).astype(BF16)
        code = jnp.concatenate([code] * QUARTERS, axis=0)
        weight = jnp.concatenate([weight.astype(BF16)] * QUARTERS, axis=0)
        for u in range(units):
            here = pl.ds(u * unit, unit)
            there = slice(u * unit, (u + 1) * unit)
            gath[here] = jnp.where(dot_nt(sel[here], code) == pick_g[here], 1.0, 0.0).astype(BF16)
            hits = dot_nt(code, sel[here]) == pick_s[:, there]
            comb[m, :, there] = jnp.where(hits, dot_nt(weight, sel[here]), 0.0).astype(BF16)

        from_input(m).wait()
        state = hbuf[m].astype(F32)
        scale = lax.rsqrt(jnp.mean(state * state, axis=-1, keepdims=True) + EPS)
        normed = (state * scale * gain_ref[...]).astype(BF16)
        for c in range(CHUNKS):
            for q in range(QUARTERS):
                at = c * cw + q * qw
                xq[q * rows : (q + 1) * rows, c * qw : (c + 1) * qw] = normed[:, at : at + qw]
        for c in range(CHUNKS):
            for u in range(units):
                here = pl.ds(u * unit, unit)
                sendbuf[m, c, here] = dot(gath[here], xq[:, c * qw : (c + 1) * qw]).astype(BF16)
            for offset in offsets:
                pe, py = peer(offset)
                out_copy_of(m, c, pe * ys + py, pe, py).start()
            recvbuf[m, c, part_of(me)] = sendbuf[m, c, part_of(me)]

    def experts(m):
        for c in range(CHUNKS):
            for offset in reversed(offsets):
                pe, py = peer(offset)
                in_copy_of(m, c, pe * ys + py, pe, py).wait_recv()
            for u in range(units):
                apart = dot(unpack[...], recvbuf[m, c, u * unit : (u + 1) * unit]).astype(BF16)
                for q in range(QUARTERS):
                    for j in range(locals_):
                        at = (q * locals_ + j) * per
                        to = c * cw + q * qw
                        xe[j, u * per : (u + 1) * per, to : to + qw] = apart[at : at + per]
            if c == 0:

                @pl.when(m == 0)
                def _():
                    for j in range(locals_):
                        loads[j][0].wait()
                        loads[j][1].wait()

            for j in range(locals_):
                held = xe[j, :, c * cw : (c + 1) * cw]
                for f in range(0, ff, 256):
                    cols = slice(f, f + 256)
                    gate = dot(held, wg[j, c * cw : (c + 1) * cw, cols])
                    upward = dot(held, wu[j, c * cw : (c + 1) * cw, cols])
                    if c > 0:
                        gate = gate + acc[0, j, :, cols]
                        upward = upward + acc[1, j, :, cols]
                    if c < CHUNKS - 1:
                        acc[0, j, :, cols] = gate
                        acc[1, j, :, cols] = upward
                    else:
                        hid[j, :, cols] = (jax.nn.silu(gate) * upward).astype(BF16)

        @pl.when(m == 0)
        def _():
            for j in range(locals_):
                loads[j][2].wait()

        for c in range(CHUNKS):
            for j in range(locals_):
                for q in range(QUARTERS):
                    to = c * cw + q * qw
                    made = dot(hid[j], wd[j, :, to : to + qw]).astype(BF16)
                    at = (q * locals_ + j) * per
                    for u in range(units):
                        stack[u, at : at + per] = made[u * per : (u + 1) * per]
            for u in range(units):
                backbuf[m, c, u * unit : (u + 1) * unit] = dot(repack[...], stack[u]).astype(BF16)
            for offset in offsets:
                pe, py = peer(offset)
                back_copy_of(m, c, pe * ys + py, pe, py).start()
            homebuf[m, c, part_of(me)] = backbuf[m, c, part_of(me)]

    def finish(m):
        for c in range(CHUNKS):
            for offset in reversed(offsets):
                pe, py = peer(offset)
                home_copy_of(m, c, pe * ys + py, pe, py).wait_recv()
            mixed = dot(comb[m], homebuf[m, c])
            for q in range(QUARTERS):
                cols = slice(c * cw + q * qw, c * cw + (q + 1) * qw)
                added = hbuf[m, :, cols].astype(F32) + mixed[q * rows : (q + 1) * rows]
                obuf[m, :, cols] = added.astype(BF16)

        @pl.when(stage < stages - 1)
        def _():
            hand_copy(m).start()

        out_copy(m).start()

    @pl.loop(0, micro + 1)
    def _(i):
        @pl.when(i > 0)
        def _():
            experts(i - 1)

        @pl.when(i < micro)
        def _():
            dispatch(i)

        @pl.when(i > 0)
        def _():
            finish(i - 1)

    @pl.loop(0, micro)
    def _(m):
        for c in range(CHUNKS):
            for offset in offsets:
                pe, py = peer(offset)
                out_copy_of(m, c, pe * ys + py, pe, py).wait_send()
                back_copy_of(m, c, pe * ys + py, pe, py).wait_send()

        @pl.when(stage < stages - 1)
        def _():
            hand_copy(m).wait_send()

        out_copy(m).wait()


def relayed(hidden_in, routes, gate_probs, norm_gain, w_gate, w_up, w_down):
    micro, rows, width = hidden_in.shape
    _, locals_, _, ff = w_gate.shape
    stages, zs, ys = (lax.axis_size(a) for a in ("pipe", "exp", "pair"))
    groups = zs * ys
    block = QUARTERS * locals_ * SLOTS
    total = groups * block
    unit = UNITS * block
    qw = width // CHUNKS // QUARTERS
    dma = pltpu.SemaphoreType.DMA
    anywhere = pl.BlockSpec(memory_space=pl.ANY)
    inside = pl.BlockSpec(memory_space=pltpu.VMEM)
    moved = pltpu.VMEM((micro, CHUNKS, total, qw), BF16)
    return pl.pallas_call(
        functools.partial(relay_kernel, stages, zs, ys),
        out_shape=jax.ShapeDtypeStruct((1, micro, rows, width), BF16),
        in_specs=[anywhere, inside, inside, inside, anywhere, anywhere, anywhere],
        out_specs=anywhere,
        scratch_shapes=[
            pltpu.VMEM((locals_, width, ff), BF16),
            pltpu.VMEM((locals_, width, ff), BF16),
            pltpu.VMEM((locals_, ff, width), BF16),
            pltpu.VMEM((micro, rows, width), BF16),
            pltpu.VMEM((micro, rows, width), BF16),
            pltpu.VMEM((QUARTERS * rows, CHUNKS * qw), BF16),
            moved,
            moved,
            moved,
            moved,
            pltpu.VMEM((locals_, groups * SLOTS, width), BF16),
            pltpu.VMEM((2, locals_, groups * SLOTS, ff), F32),
            pltpu.VMEM((locals_, groups * SLOTS, ff), BF16),
            pltpu.VMEM((groups // UNITS, unit, qw), BF16),
            pltpu.VMEM((total, LANES), BF16),
            pltpu.VMEM((total, LANES), F32),
            pltpu.VMEM((QUARTERS * rows, total), F32),
            pltpu.VMEM((total, LANES), BF16),
            pltpu.VMEM((micro, QUARTERS * rows, total), BF16),
            pltpu.VMEM((unit, unit), BF16),
            pltpu.VMEM((unit, unit), BF16),
            dma((3 * locals_,)),
            dma((micro,)),
            dma((micro,)),
            dma((micro,)),
            dma((micro, CHUNKS, groups)),
            dma((micro, CHUNKS, groups)),
            dma((micro, CHUNKS, groups)),
            dma((micro, CHUNKS, groups)),
        ],
        compiler_params=pltpu.CompilerParams(
            collective_id=0, has_side_effects=True, vmem_limit_bytes=VMEM_LIMIT
        ),
    )(hidden_in, routes, gate_probs, norm_gain, w_gate, w_up, w_down)


def solution(mesh):
    in_specs = (
        P(None, ("exp", "pair"), None),
        P("pipe", None, ("exp", "pair"), None),
        P("pipe", None, ("exp", "pair"), None),
        P("pipe", None),
        P("pipe", ("exp", "pair"), None, None),
        P("pipe", ("exp", "pair"), None, None),
        P("pipe", ("exp", "pair"), None, None),
    )
    out_specs = P("pipe", None, ("exp", "pair"), None)
    return jax.shard_map(
        relayed, mesh=mesh, in_specs=in_specs, out_specs=out_specs, check_vma=False
    )
```

```python
import functools

import jax
import jax.numpy as jnp
from jax import lax
from jax.experimental import pallas as pl
from jax.experimental.pallas import tpu as pltpu
from jax.sharding import PartitionSpec as P

EPS = 1e-06
MESH = pl.DeviceIdType.MESH
F32 = jnp.float32
BF16 = jnp.bfloat16
VMEM_LIMIT = 63 * 1024 * 1024
SLOTS = 6
SIDE = 4
STRIPS = 8
LANES = 128
UNITS = 8
ORDERED = (False, False, False, False)


def fdiv(value, n):
    return jnp.floor((value + 0.5) * (1.0 / n))


def iota(shape, axis):
    return lax.broadcasted_iota(jnp.int32, shape, axis).astype(F32)


def dot(a, b):
    return jnp.dot(a, b, preferred_element_type=F32)


def dot_nt(a, b):
    return lax.dot_general(a, b, (((1,), (1,)), ((), ())), preferred_element_type=F32)


def relay_kernel(
    stages,
    zs,
    ys,
    hidden_ref,
    routes_ref,
    probs_ref,
    gain_ref,
    wgate_ref,
    wup_ref,
    wdown_ref,
    out_ref,
    wg,
    wu,
    wd,
    hbuf,
    obuf,
    xq,
    sendbuf,
    recvbuf,
    backbuf,
    homebuf,
    xe,
    hid,
    stack,
    sel,
    pick_g,
    pick_s,
    code,
    gath,
    comb,
    unpack,
    repack,
    w_sem,
    h_sem,
    hs_sem,
    o_sem,
    a_sem,
    ar_sem,
    b_sem,
    br_sem,
):
    micro, rows, width = hbuf.shape
    locals_, _, ff = wg.shape
    groups = zs * ys
    block = STRIPS * SLOTS
    qw = width // STRIPS
    unit = UNITS * block
    units = groups // UNITS
    per = UNITS * SLOTS

    stage = lax.axis_index("pipe")
    e_idx = lax.axis_index("exp")
    y = lax.axis_index("pair")
    me = e_idx * ys + y
    cx = lax.div(e_idx, SIDE)
    cz = lax.rem(e_idx, SIDE)

    def ring(d):
        return min(d, SIDE - d)

    offsets = [
        (dx, dz, dy)
        for dx in range(zs // SIDE)
        for dz in range(SIDE)
        for dy in range(ys)
        if dx or dz or dy
    ]
    offsets.sort(key=lambda o: -(ring(o[0]) + ring(o[1]) + o[2]))

    def peer(offset):
        dx, dz, dy = offset
        px = lax.rem(cx + dx, zs // SIDE)
        pz = lax.rem(cz + dz, SIDE)
        return px * SIDE + pz, lax.rem(y + dy, ys)

    loads = []
    for j in range(locals_):
        loads.append(
            (
                pltpu.make_async_copy(wgate_ref.at[0, j], wg.at[j], w_sem.at[3 * j]),
                pltpu.make_async_copy(wup_ref.at[0, j], wu.at[j], w_sem.at[3 * j + 1]),
                pltpu.make_async_copy(wdown_ref.at[0, j], wd.at[j], w_sem.at[3 * j + 2]),
            )
        )

    def from_input(m):
        return pltpu.make_async_copy(hidden_ref.at[m], hbuf.at[m], h_sem.at[m])

    @pl.when(stage == 0)
    def _():
        for m in range(micro):
            from_input(m).start()

    for j in range(locals_):
        for load in loads[j]:
            load.start()

    barrier = pltpu.get_barrier_semaphore()
    for offset in offsets:
        pe, py = peer(offset)
        pl.semaphore_signal(barrier, inc=1, device_id={"exp": pe, "pair": py}, device_id_type=MESH)

    @pl.when(stage > 0)
    def _():
        pl.semaphore_signal(barrier, inc=1, device_id={"pipe": stage - 1}, device_id_type=MESH)

    @pl.when(stage < stages - 1)
    def _():
        pl.semaphore_signal(barrier, inc=1, device_id={"pipe": stage + 1}, device_id_type=MESH)

    def row_parts(index):
        d = fdiv(index, block)
        r = index - block * d
        q = fdiv(r, SLOTS)
        return d, q, r - SLOTS * q

    for u in range(units):
        here = pl.ds(u * unit, unit)
        d, _, _ = row_parts(iota((unit, LANES), 0) + u * unit)
        lane = iota((unit, LANES), 1)
        for j in range(locals_):
            sel[j, here] = jnp.where(lane == locals_ * d + j, 1.0, 0.0).astype(BF16)
        _, q, s = row_parts(iota((unit, STRIPS * rows), 0) + u * unit)
        at = iota((unit, STRIPS * rows), 1)
        pick_g[here] = jnp.where(fdiv(at, rows) == q, s + 1.0, -1.0)
        _, q, s = row_parts(iota((STRIPS * rows, unit), 1) + u * unit)
        at = iota((STRIPS * rows, unit), 0)
        pick_s[:, u * unit : (u + 1) * unit] = jnp.where(fdiv(at, rows) == q, s + 1.0, -1.0)
    d, q, s = row_parts(iota((unit, unit), 1))
    unpack[...] = jnp.where(iota((unit, unit), 0) == q * per + d * SLOTS + s, 1.0, 0.0).astype(BF16)
    d, q, s = row_parts(iota((unit, unit), 0))
    repack[...] = jnp.where(iota((unit, unit), 1) == q * per + d * SLOTS + s, 1.0, 0.0).astype(BF16)

    linked = (stage > 0).astype(jnp.int32) + (stage < stages - 1).astype(jnp.int32)
    pl.semaphore_wait(barrier, len(offsets) + linked)

    def part_of(at):
        return pl.ds(pl.multiple_of(at * block, block), block)

    def out_copy_of(m, c, at, pe, py):
        return pltpu.make_async_remote_copy(
            src_ref=sendbuf.at[m, c, part_of(at)],
            dst_ref=recvbuf.at[m, c, part_of(me)],
            send_sem=a_sem.at[m, c, at],
            recv_sem=ar_sem.at[m, c, me],
            device_id={"exp": pe, "pair": py},
            device_id_type=MESH,
        )

    def in_copy_of(m, c, at, pe, py):
        return pltpu.make_async_remote_copy(
            src_ref=sendbuf.at[m, c, part_of(at)],
            dst_ref=recvbuf.at[m, c, part_of(at)],
            send_sem=a_sem.at[m, c, at],
            recv_sem=ar_sem.at[m, c, at],
            device_id={"exp": pe, "pair": py},
            device_id_type=MESH,
        )

    def back_copy_of(m, c, at, pe, py):
        return pltpu.make_async_remote_copy(
            src_ref=backbuf.at[m, c, part_of(at)],
            dst_ref=homebuf.at[m, c, part_of(me)],
            send_sem=b_sem.at[m, c, at],
            recv_sem=br_sem.at[m, c, me],
            device_id={"exp": pe, "pair": py},
            device_id_type=MESH,
        )

    def home_copy_of(m, c, at, pe, py):
        return pltpu.make_async_remote_copy(
            src_ref=backbuf.at[m, c, part_of(at)],
            dst_ref=homebuf.at[m, c, part_of(at)],
            send_sem=b_sem.at[m, c, at],
            recv_sem=br_sem.at[m, c, at],
            device_id={"exp": pe, "pair": py},
            device_id_type=MESH,
        )

    def hand_copy(m):
        return pltpu.make_async_remote_copy(
            src_ref=obuf.at[m],
            dst_ref=hbuf.at[m],
            send_sem=hs_sem.at[m],
            recv_sem=h_sem.at[m],
            device_id={"pipe": stage + 1},
            device_id_type=MESH,
        )

    def out_copy(m):
        return pltpu.make_async_copy(obuf.at[m], out_ref.at[0, m], o_sem.at[m])

    earlier = (iota((rows, rows), 0) >= iota((rows, rows), 1)).astype(F32).astype(BF16)

    def out_sent(m, j):
        for offset in offsets:
            pe, py = peer(offset)
            out_copy_of(m, j, pe * ys + py, pe, py).wait_send()

    def back_sent(m, j):
        for offset in offsets:
            pe, py = peer(offset)
            back_copy_of(m, j, pe * ys + py, pe, py).wait_send()

    last = locals_ - 1

    def prepare(m):
        chosen = routes_ref[0, m]
        probs = probs_ref[0, m]
        normal = probs / jnp.sum(probs, axis=-1, keepdims=True)
        lane = lax.broadcasted_iota(jnp.int32, (rows, LANES), 1)
        mask = jnp.zeros((rows, LANES), F32)
        weight = jnp.zeros((rows, LANES), F32)
        for k in range(chosen.shape[1]):
            hit = lane == chosen[:, k : k + 1]
            mask = mask + jnp.where(hit, 1.0, 0.0)
            weight = weight + jnp.where(hit, normal[:, k : k + 1], 0.0)
        ranks = (mask * dot(earlier, mask.astype(BF16))).astype(BF16)
        code[...] = jnp.concatenate([ranks] * STRIPS, axis=0)
        weight = jnp.concatenate([weight.astype(BF16)] * STRIPS, axis=0)
        for j in range(locals_):
            for u in range(units):
                here = pl.ds(u * unit, unit)
                there = slice(u * unit, (u + 1) * unit)
                found = dot_nt(sel[j, here], code[...]) == pick_g[here]
                gath[j, here] = jnp.where(found, 1.0, 0.0).astype(BF16)
                hits = dot_nt(code[...], sel[j, here]) == pick_s[:, there]
                shares = jnp.where(hits, dot_nt(weight, sel[j, here]), 0.0)
                comb[lax.rem(m, 2), j, :, there] = shares.astype(BF16)

        from_input(m).wait()
        state = hbuf[m].astype(F32)
        scale = lax.rsqrt(jnp.mean(state * state, axis=-1, keepdims=True) + EPS)
        normed = (state * scale * gain_ref[...]).astype(BF16)
        for q in range(STRIPS):
            xq[q * rows : (q + 1) * rows] = normed[:, q * qw : (q + 1) * qw]

    def dispatch(m, j):
        for u in range(units):
            here = pl.ds(u * unit, unit)
            sendbuf[m, j, here] = dot(gath[j, here], xq[...]).astype(BF16)
        recvbuf[m, j, part_of(me)] = sendbuf[m, j, part_of(me)]
        if j > 0:
            if ORDERED[1]:
                out_sent(m, j - 1)
        elif ORDERED[0]:

            @pl.when(m > 0)
            def _():
                back_sent(m - 1, last)

        for offset in offsets:
            pe, py = peer(offset)
            out_copy_of(m, j, pe * ys + py, pe, py).start()

    def expert(m, j):
        for offset in reversed(offsets):
            pe, py = peer(offset)
            in_copy_of(m, j, pe * ys + py, pe, py).wait_recv()
        for u in range(units):
            apart = dot(unpack[...], recvbuf[m, j, u * unit : (u + 1) * unit]).astype(BF16)
            for q in range(STRIPS):
                xe[u * per : (u + 1) * per, q * qw : (q + 1) * qw] = apart[q * per : (q + 1) * per]

        @pl.when(m == 0)
        def _():
            for load in loads[j]:
                load.wait()

        held = xe[...]
        for f in range(0, ff, 256):
            cols = slice(f, f + 256)
            gate = dot(held, wg[j, :, cols])
            upward = dot(held, wu[j, :, cols])
            hid[:, cols] = (jax.nn.silu(gate) * upward).astype(BF16)
        for q in range(STRIPS):
            made = dot(hid[...], wd[j, :, q * qw : (q + 1) * qw]).astype(BF16)
            for u in range(units):
                stack[u, q * per : (q + 1) * per] = made[u * per : (u + 1) * per]
        for u in range(units):
            backbuf[m, j, u * unit : (u + 1) * unit] = dot(repack[...], stack[u]).astype(BF16)
        homebuf[m, j, part_of(me)] = backbuf[m, j, part_of(me)]
        if j > 0:
            if ORDERED[3]:
                back_sent(m, j - 1)
        elif ORDERED[2]:
            out_sent(m, last)
        for offset in offsets:
            pe, py = peer(offset)
            back_copy_of(m, j, pe * ys + py, pe, py).start()

    def finish(m):
        mixed = jnp.zeros((STRIPS * rows, qw), F32)
        for j in range(locals_):
            for offset in reversed(offsets):
                pe, py = peer(offset)
                home_copy_of(m, j, pe * ys + py, pe, py).wait_recv()
            mixed = mixed + dot(comb[lax.rem(m, 2), j], homebuf[m, j])
        for q in range(STRIPS):
            cols = slice(q * qw, (q + 1) * qw)
            added = hbuf[m, :, cols].astype(F32) + mixed[q * rows : (q + 1) * rows]
            obuf[m, :, cols] = added.astype(BF16)

        @pl.when(stage < stages - 1)
        def _():
            hand_copy(m).start()

        out_copy(m).start()

    @pl.loop(0, micro + 1)
    def _(i):
        @pl.when(i < micro)
        def _():
            prepare(i)
            dispatch(i, 0)

        @pl.when(i > 0)
        def _():
            finish(i - 1)

        @pl.when(i < micro)
        def _():
            for j in range(1, locals_):
                dispatch(i, j)
            for j in range(locals_):
                expert(i, j)

    if ORDERED[0]:
        back_sent(micro - 1, last)

    @pl.loop(0, micro)
    def _(m):
        if not ORDERED[0]:
            back_sent(m, last)
        if not ORDERED[1]:
            for j in range(last):
                out_sent(m, j)
        if not ORDERED[2]:
            out_sent(m, last)
        if not ORDERED[3]:
            for j in range(last):
                back_sent(m, j)

        @pl.when(stage < stages - 1)
        def _():
            hand_copy(m).wait_send()

        out_copy(m).wait()


def relayed(hidden_in, routes, gate_probs, norm_gain, w_gate, w_up, w_down):
    micro, rows, width = hidden_in.shape
    _, locals_, _, ff = w_gate.shape
    stages, zs, ys = (lax.axis_size(a) for a in ("pipe", "exp", "pair"))
    groups = zs * ys
    block = STRIPS * SLOTS
    total = groups * block
    unit = UNITS * block
    qw = width // STRIPS
    spread = STRIPS * rows
    dma = pltpu.SemaphoreType.DMA
    anywhere = pl.BlockSpec(memory_space=pl.ANY)
    inside = pl.BlockSpec(memory_space=pltpu.VMEM)
    moved = pltpu.VMEM((micro, locals_, total, qw), BF16)
    return pl.pallas_call(
        functools.partial(relay_kernel, stages, zs, ys),
        out_shape=jax.ShapeDtypeStruct((1, micro, rows, width), BF16),
        in_specs=[anywhere, inside, inside, inside, anywhere, anywhere, anywhere],
        out_specs=anywhere,
        scratch_shapes=[
            pltpu.VMEM((locals_, width, ff), BF16),
            pltpu.VMEM((locals_, width, ff), BF16),
            pltpu.VMEM((locals_, ff, width), BF16),
            pltpu.VMEM((micro, rows, width), BF16),
            pltpu.VMEM((micro, rows, width), BF16),
            pltpu.VMEM((spread, qw), BF16),
            moved,
            moved,
            moved,
            moved,
            pltpu.VMEM((groups * SLOTS, width), BF16),
            pltpu.VMEM((groups * SLOTS, ff), BF16),
            pltpu.VMEM((groups // UNITS, unit, qw), BF16),
            pltpu.VMEM((locals_, total, LANES), BF16),
            pltpu.VMEM((total, spread), F32),
            pltpu.VMEM((spread, total), F32),
            pltpu.VMEM((spread, LANES), BF16),
            pltpu.VMEM((locals_, total, spread), BF16),
            pltpu.VMEM((2, locals_, spread, total), BF16),
            pltpu.VMEM((unit, unit), BF16),
            pltpu.VMEM((unit, unit), BF16),
            dma((3 * locals_,)),
            dma((micro,)),
            dma((micro,)),
            dma((micro,)),
            dma((micro, locals_, groups)),
            dma((micro, locals_, groups)),
            dma((micro, locals_, groups)),
            dma((micro, locals_, groups)),
        ],
        compiler_params=pltpu.CompilerParams(
            collective_id=0, has_side_effects=True, vmem_limit_bytes=VMEM_LIMIT
        ),
    )(hidden_in, routes, gate_probs, norm_gain, w_gate, w_up, w_down)


def solution(mesh):
    in_specs = (
        P(None, ("exp", "pair"), None),
        P("pipe", None, ("exp", "pair"), None),
        P("pipe", None, ("exp", "pair"), None),
        P("pipe", None),
        P("pipe", ("exp", "pair"), None, None),
        P("pipe", ("exp", "pair"), None, None),
        P("pipe", ("exp", "pair"), None, None),
    )
    out_specs = P("pipe", None, ("exp", "pair"), None)
    return jax.shard_map(
        relayed, mesh=mesh, in_specs=in_specs, out_specs=out_specs, check_vma=False
    )
```

```python
import functools

import jax
import jax.numpy as jnp
from jax import lax
from jax.experimental import pallas as pl
from jax.experimental.pallas import tpu as pltpu
from jax.sharding import PartitionSpec as P

EPS = 1e-06
MESH = pl.DeviceIdType.MESH
F32 = jnp.float32
BF16 = jnp.bfloat16
VMEM_LIMIT = 63 * 1024 * 1024
SLOTS = 6
SIDE = 4
STRIPS = 8
LANES = 128
UNITS = 8
CUTS = 4
PLACES = ((0, 2, 2), (0, 2, 2), (0, 2, 2), (0, 2, 2))
ORDERED = (False, False, False, False)


def fdiv(value, n):
    return jnp.floor((value + 0.5) * (1.0 / n))


def iota(shape, axis):
    return lax.broadcasted_iota(jnp.int32, shape, axis).astype(F32)


def dot(a, b):
    return jnp.dot(a, b, preferred_element_type=F32)


def dot_nt(a, b):
    return lax.dot_general(a, b, (((1,), (1,)), ((), ())), preferred_element_type=F32)


def relay_kernel(
    stages,
    zs,
    ys,
    hidden_ref,
    routes_hbm,
    probs_hbm,
    gain_hbm,
    wgate_ref,
    wup_ref,
    wdown_ref,
    out_ref,
    routes_ref,
    probs_ref,
    gain_ref,
    wg,
    wu,
    wd,
    hbuf,
    obuf,
    xq,
    sendbuf,
    recvbuf,
    backbuf,
    homebuf,
    xe,
    hid,
    stack,
    sel,
    pick_g,
    pick_s,
    code,
    gath,
    comb,
    unpack,
    repack,
    i_sem,
    w_sem,
    h_sem,
    hs_sem,
    o_sem,
    a_sem,
    ar_sem,
    b_sem,
    br_sem,
):
    micro, rows, width = hbuf.shape
    locals_, _, ff = wg.shape
    groups = zs * ys
    block = STRIPS * SLOTS
    qw = width // STRIPS
    unit = UNITS * block
    units = groups // UNITS
    per = UNITS * SLOTS

    stage = lax.axis_index("pipe")
    e_idx = lax.axis_index("exp")
    y = lax.axis_index("pair")
    me = e_idx * ys + y
    cx = lax.div(e_idx, SIDE)
    cz = lax.rem(e_idx, SIDE)

    def ring(d):
        return min(d, SIDE - d)

    offsets = [
        (dx, dz, dy)
        for dx in range(zs // SIDE)
        for dz in range(SIDE)
        for dy in range(ys)
        if dx or dz or dy
    ]
    offsets.sort(key=lambda o: -(ring(o[0]) + ring(o[1]) + o[2]))

    def peer(offset):
        dx, dz, dy = offset
        px = lax.rem(cx + dx, zs // SIDE)
        pz = lax.rem(cz + dz, SIDE)
        return px * SIDE + pz, lax.rem(y + dy, ys)

    loads = []
    for j in range(locals_):
        pieces = []
        for k, (source, target) in enumerate(
            ((wgate_ref, wg), (wup_ref, wu), (wdown_ref, wd))
        ):
            tall = target.shape[1] // CUTS
            for cut in range(CUTS):
                part = pl.ds(cut * tall, tall)
                sem = w_sem.at[(3 * j + k) * CUTS + cut]
                pieces.append(
                    pltpu.make_async_copy(source.at[0, j, part], target.at[j, part], sem)
                )
        loads.append(pieces)

    def from_input(m):
        return pltpu.make_async_copy(hidden_ref.at[m], hbuf.at[m], h_sem.at[m])

    small = (
        pltpu.make_async_copy(routes_hbm, routes_ref, i_sem.at[0]),
        pltpu.make_async_copy(probs_hbm, probs_ref, i_sem.at[1]),
        pltpu.make_async_copy(gain_hbm, gain_ref, i_sem.at[2]),
    )
    for load in small:
        load.start()

    @pl.when(stage == 0)
    def _():
        for m in range(micro):
            from_input(m).start()

    for j in range(locals_):
        for load in loads[j]:
            load.start()

    barrier = pltpu.get_barrier_semaphore()
    for offset in offsets:
        pe, py = peer(offset)
        pl.semaphore_signal(barrier, inc=1, device_id={"exp": pe, "pair": py}, device_id_type=MESH)

    @pl.when(stage > 0)
    def _():
        pl.semaphore_signal(barrier, inc=1, device_id={"pipe": stage - 1}, device_id_type=MESH)

    @pl.when(stage < stages - 1)
    def _():
        pl.semaphore_signal(barrier, inc=1, device_id={"pipe": stage + 1}, device_id_type=MESH)

    def row_parts(index):
        d = fdiv(index, block)
        r = index - block * d
        q = fdiv(r, SLOTS)
        return d, q, r - SLOTS * q

    down, _, _ = row_parts(iota((unit, 1), 0))
    lane = iota((unit, LANES), 1)
    base = lane - locals_ * down
    for j in range(locals_):
        for u in range(units):
            first = locals_ * u * UNITS + j
            sel[j, pl.ds(u * unit, unit)] = jnp.where(base == first, 1.0, 0.0).astype(BF16)
    _, q, s = row_parts(iota((unit, 1), 0))
    pick_g[...] = jnp.where(fdiv(iota((1, STRIPS * rows), 1), rows) == q, s + 1.0, -1.0)


    def part_of(at):
        return pl.ds(pl.multiple_of(at * block, block), block)

    def out_copy_of(m, c, at, pe, py):
        return pltpu.make_async_remote_copy(
            src_ref=sendbuf.at[m, c, part_of(at)],
            dst_ref=recvbuf.at[m, c, part_of(me)],
            send_sem=a_sem.at[m, c, at],
            recv_sem=ar_sem.at[m, c, me],
            device_id={"exp": pe, "pair": py},
            device_id_type=MESH,
        )

    def in_copy_of(m, c, at, pe, py):
        return pltpu.make_async_remote_copy(
            src_ref=sendbuf.at[m, c, part_of(at)],
            dst_ref=recvbuf.at[m, c, part_of(at)],
            send_sem=a_sem.at[m, c, at],
            recv_sem=ar_sem.at[m, c, at],
            device_id={"exp": pe, "pair": py},
            device_id_type=MESH,
        )

    def back_copy_of(m, c, at, pe, py):
        return pltpu.make_async_remote_copy(
            src_ref=backbuf.at[m, c, part_of(at)],
            dst_ref=homebuf.at[m, c, part_of(me)],
            send_sem=b_sem.at[m, c, at],
            recv_sem=br_sem.at[m, c, me],
            device_id={"exp": pe, "pair": py},
            device_id_type=MESH,
        )

    def home_copy_of(m, c, at, pe, py):
        return pltpu.make_async_remote_copy(
            src_ref=backbuf.at[m, c, part_of(at)],
            dst_ref=homebuf.at[m, c, part_of(at)],
            send_sem=b_sem.at[m, c, at],
            recv_sem=br_sem.at[m, c, at],
            device_id={"exp": pe, "pair": py},
            device_id_type=MESH,
        )

    def hand_copy(m):
        return pltpu.make_async_remote_copy(
            src_ref=obuf.at[m],
            dst_ref=hbuf.at[m],
            send_sem=hs_sem.at[m],
            recv_sem=h_sem.at[m],
            device_id={"pipe": stage + 1},
            device_id_type=MESH,
        )

    def out_copy(m):
        return pltpu.make_async_copy(obuf.at[m], out_ref.at[0, m], o_sem.at[m])

    earlier = (iota((rows, rows), 0) >= iota((rows, rows), 1)).astype(F32).astype(BF16)

    def out_sent(m, j):
        for offset in offsets:
            pe, py = peer(offset)
            out_copy_of(m, j, pe * ys + py, pe, py).wait_send()

    def back_sent(m, j):
        for offset in offsets:
            pe, py = peer(offset)
            back_copy_of(m, j, pe * ys + py, pe, py).wait_send()

    last = locals_ - 1

    def settle():
        _, q, s = row_parts(iota((1, unit), 1))
        pick_s[...] = jnp.where(fdiv(iota((STRIPS * rows, 1), 0), rows) == q, s + 1.0, -1.0)
        d, q, s = row_parts(iota((1, unit), 1))
        moved_to = q * per + d * SLOTS + s
        unpack[...] = jnp.where(iota((unit, unit), 0) == moved_to, 1.0, 0.0).astype(BF16)
        d, q, s = row_parts(iota((unit, 1), 0))
        moved_to = q * per + d * SLOTS + s
        repack[...] = jnp.where(iota((unit, unit), 1) == moved_to, 1.0, 0.0).astype(BF16)

    def route(m):
        chosen = routes_ref[0, m]
        probs = probs_ref[0, m]
        normal = probs / jnp.sum(probs, axis=-1, keepdims=True)
        lane = lax.broadcasted_iota(jnp.int32, (rows, LANES), 1)
        mask = jnp.zeros((rows, LANES), F32)
        weight = jnp.zeros((rows, LANES), F32)
        for k in range(chosen.shape[1]):
            hit = lane == chosen[:, k : k + 1]
            mask = mask + jnp.where(hit, 1.0, 0.0)
            weight = weight + jnp.where(hit, normal[:, k : k + 1], 0.0)
        ranks = (mask * dot(earlier, mask.astype(BF16))).astype(BF16)
        code[0] = jnp.concatenate([ranks] * STRIPS, axis=0)
        code[1] = jnp.concatenate([weight.astype(BF16)] * STRIPS, axis=0)
        gather(0)

    def gather(j):
        for u in range(units):
            here = pl.ds(u * unit, unit)
            found = dot_nt(sel[j, here], code[0]) == pick_g[...]
            gath[j, here] = jnp.where(found, 1.0, 0.0).astype(BF16)

    def weigh(m):
        for j in range(locals_):
            for u in range(units):
                here = pl.ds(u * unit, unit)
                there = slice(u * unit, (u + 1) * unit)
                hits = dot_nt(code[0], sel[j, here]) == pick_s[...]
                shares = jnp.where(hits, dot_nt(code[1], sel[j, here]), 0.0)
                comb[lax.rem(m, 2), j, :, there] = shares.astype(BF16)

    def prepare(m):
        from_input(m).wait()
        state = hbuf[m].astype(F32)
        scale = lax.rsqrt(jnp.mean(state * state, axis=-1, keepdims=True) + EPS)
        normed = (state * scale * gain_ref[...]).astype(BF16)
        for q in range(STRIPS):
            xq[q * rows : (q + 1) * rows] = normed[:, q * qw : (q + 1) * qw]

    def dispatch(m, j):
        for u in range(units):
            here = pl.ds(u * unit, unit)
            sendbuf[m, j, here] = dot(gath[j, here], xq[...]).astype(BF16)
        recvbuf[m, j, part_of(me)] = sendbuf[m, j, part_of(me)]
        if j > 0:
            if ORDERED[1]:
                out_sent(m, j - 1)
        elif ORDERED[0]:

            @pl.when(m > 0)
            def _():
                back_sent(m - 1, last)

        for offset in offsets:
            pe, py = peer(offset)
            out_copy_of(m, j, pe * ys + py, pe, py).start()

    def expert(m, j):
        for offset in reversed(offsets):
            pe, py = peer(offset)
            in_copy_of(m, j, pe * ys + py, pe, py).wait_recv()
        for u in range(units):
            apart = dot(unpack[...], recvbuf[m, j, u * unit : (u + 1) * unit]).astype(BF16)
            for q in range(STRIPS):
                xe[u * per : (u + 1) * per, q * qw : (q + 1) * qw] = apart[q * per : (q + 1) * per]

        @pl.when(m == 0)
        def _():
            for load in loads[j]:
                load.wait()

        held = xe[...]
        for f in range(0, ff, 256):
            cols = slice(f, f + 256)
            gate = dot(held, wg[j, :, cols])
            upward = dot(held, wu[j, :, cols])
            hid[:, cols] = (jax.nn.silu(gate) * upward).astype(BF16)
        for q in range(STRIPS):
            made = dot(hid[...], wd[j, :, q * qw : (q + 1) * qw]).astype(BF16)
            for u in range(units):
                stack[u, q * per : (q + 1) * per] = made[u * per : (u + 1) * per]
        for u in range(units):
            backbuf[m, j, u * unit : (u + 1) * unit] = dot(repack[...], stack[u]).astype(BF16)
        homebuf[m, j, part_of(me)] = backbuf[m, j, part_of(me)]
        if j > 0:
            if ORDERED[3]:
                back_sent(m, j - 1)
        elif ORDERED[2]:
            out_sent(m, last)
        for offset in offsets:
            pe, py = peer(offset)
            back_copy_of(m, j, pe * ys + py, pe, py).start()

    def finish(m):
        mixed = jnp.zeros((STRIPS * rows, qw), F32)
        for j in range(locals_):
            for offset in reversed(offsets):
                pe, py = peer(offset)
                home_copy_of(m, j, pe * ys + py, pe, py).wait_recv()
            mixed = mixed + dot(comb[lax.rem(m, 2), j], homebuf[m, j])
        for q in range(STRIPS):
            cols = slice(q * qw, (q + 1) * qw)
            added = hbuf[m, :, cols].astype(F32) + mixed[q * rows : (q + 1) * rows]
            obuf[m, :, cols] = added.astype(BF16)

        @pl.when(stage < stages - 1)
        def _():
            hand_copy(m).start()

        out_copy(m).start()

    for load in small:
        load.wait()
    route(0)
    linked = (stage > 0).astype(jnp.int32) + (stage < stages - 1).astype(jnp.int32)
    pl.semaphore_wait(barrier, len(offsets) + linked)

    @pl.loop(0, micro + 1)
    def _(i):
        def finish_at(place):
            now = i == micro if place == 0 else i < 0
            for at in range(stages):
                for step in range(micro - 1):
                    if PLACES[at][step] == place:
                        now = jnp.logical_or(now, jnp.logical_and(stage == at, i == step + 1))

            @pl.when(now)
            def _():
                finish(i - 1)

        finish_at(0)

        @pl.when(i < micro)
        def _():
            prepare(i)

        finish_at(1)

        @pl.when(i < micro)
        def _():
            dispatch(i, 0)

        finish_at(2)

        @pl.when(i < micro)
        def _():
            for j in range(1, locals_):

                @pl.when(i == 0)
                def _():
                    gather(j)

                dispatch(i, j)

        finish_at(3)

        @pl.when(i < micro)
        def _():
            pl.when(i == 0)(settle)
            weigh(i)
            for j in range(locals_):
                expert(i, j)

        @pl.when(i < micro - 1)
        def _():
            route(i + 1)
            for j in range(1, locals_):
                gather(j)

    if ORDERED[0]:
        back_sent(micro - 1, last)

    @pl.loop(0, micro)
    def _(m):
        if not ORDERED[0]:
            back_sent(m, last)
        if not ORDERED[1]:
            for j in range(last):
                out_sent(m, j)
        if not ORDERED[2]:
            out_sent(m, last)
        if not ORDERED[3]:
            for j in range(last):
                back_sent(m, j)

        @pl.when(stage < stages - 1)
        def _():
            hand_copy(m).wait_send()

        out_copy(m).wait()


def relayed(hidden_in, routes, gate_probs, norm_gain, w_gate, w_up, w_down):
    micro, rows, width = hidden_in.shape
    _, locals_, _, ff = w_gate.shape
    stages, zs, ys = (lax.axis_size(a) for a in ("pipe", "exp", "pair"))
    groups = zs * ys
    block = STRIPS * SLOTS
    total = groups * block
    unit = UNITS * block
    qw = width // STRIPS
    spread = STRIPS * rows
    dma = pltpu.SemaphoreType.DMA
    anywhere = pl.BlockSpec(memory_space=pl.ANY)
    moved = pltpu.VMEM((micro, locals_, total, qw), BF16)
    return pl.pallas_call(
        functools.partial(relay_kernel, stages, zs, ys),
        out_shape=jax.ShapeDtypeStruct((1, micro, rows, width), BF16),
        in_specs=[anywhere] * 7,
        out_specs=anywhere,
        scratch_shapes=[
            pltpu.VMEM(routes.shape, jnp.int32),
            pltpu.VMEM(gate_probs.shape, F32),
            pltpu.VMEM(norm_gain.shape, F32),
            pltpu.VMEM((locals_, width, ff), BF16),
            pltpu.VMEM((locals_, width, ff), BF16),
            pltpu.VMEM((locals_, ff, width), BF16),
            pltpu.VMEM((micro, rows, width), BF16),
            pltpu.VMEM((micro, rows, width), BF16),
            pltpu.VMEM((spread, qw), BF16),
            moved,
            moved,
            moved,
            moved,
            pltpu.VMEM((groups * SLOTS, width), BF16),
            pltpu.VMEM((groups * SLOTS, ff), BF16),
            pltpu.VMEM((groups // UNITS, unit, qw), BF16),
            pltpu.VMEM((locals_, total, LANES), BF16),
            pltpu.VMEM((unit, spread), F32),
            pltpu.VMEM((spread, unit), F32),
            pltpu.VMEM((2, spread, LANES), BF16),
            pltpu.VMEM((locals_, total, spread), BF16),
            pltpu.VMEM((2, locals_, spread, total), BF16),
            pltpu.VMEM((unit, unit), BF16),
            pltpu.VMEM((unit, unit), BF16),
            dma((3,)),
            dma((3 * locals_ * CUTS,)),
            dma((micro,)),
            dma((micro,)),
            dma((micro,)),
            dma((micro, locals_, groups)),
            dma((micro, locals_, groups)),
            dma((micro, locals_, groups)),
            dma((micro, locals_, groups)),
        ],
        compiler_params=pltpu.CompilerParams(
            collective_id=0, has_side_effects=True, vmem_limit_bytes=VMEM_LIMIT
        ),
    )(hidden_in, routes, gate_probs, norm_gain, w_gate, w_up, w_down)


def solution(mesh):
    in_specs = (
        P(None, ("exp", "pair"), None),
        P("pipe", None, ("exp", "pair"), None),
        P("pipe", None, ("exp", "pair"), None),
        P("pipe", None),
        P("pipe", ("exp", "pair"), None, None),
        P("pipe", ("exp", "pair"), None, None),
        P("pipe", ("exp", "pair"), None, None),
    )
    out_specs = P("pipe", None, ("exp", "pair"), None)
    return jax.shard_map(
        relayed, mesh=mesh, in_specs=in_specs, out_specs=out_specs, check_vma=False
    )
```

```python
import functools

import jax
import jax.numpy as jnp
from jax import lax
from jax.experimental import pallas as pl
from jax.experimental.pallas import tpu as pltpu
from jax.sharding import PartitionSpec as P

EPS = 1e-06
MESH = pl.DeviceIdType.MESH
F32 = jnp.float32
BF16 = jnp.bfloat16
VMEM_LIMIT = 63 * 1024 * 1024
SLOTS = 6
SIDE = 4
STRIPS = 8
LANES = 128
UNITS = 8
CUTS = 4
PLACES = ((0, 2, 2), (0, 2, 2), (0, 2, 2), (0, 2, 2))
ORDERED = (False, False, False, False)


def fdiv(value, n):
    return jnp.floor((value + 0.5) * (1.0 / n))


def iota(shape, axis):
    return lax.broadcasted_iota(jnp.int32, shape, axis).astype(F32)


def dot(a, b):
    return jnp.dot(a, b, preferred_element_type=F32)


def dot_nt(a, b):
    return lax.dot_general(a, b, (((1,), (1,)), ((), ())), preferred_element_type=F32)


def relay_kernel(
    stages,
    zs,
    ys,
    hidden_ref,
    routes_hbm,
    probs_hbm,
    gain_hbm,
    wgate_ref,
    wup_ref,
    wdown_ref,
    out_ref,
    routes_ref,
    probs_ref,
    gain_ref,
    wg,
    wu,
    wd,
    hbuf,
    obuf,
    xq,
    sendbuf,
    recvbuf,
    backbuf,
    homebuf,
    xe,
    hid,
    stack,
    sel,
    pick_g,
    pick_s,
    code,
    gath,
    comb,
    unpack,
    repack,
    i_sem,
    w_sem,
    h_sem,
    hs_sem,
    o_sem,
    a_sem,
    ar_sem,
    b_sem,
    br_sem,
):
    micro, rows, width = hbuf.shape
    locals_, _, ff = wg.shape
    groups = zs * ys
    block = STRIPS * SLOTS
    qw = width // STRIPS
    unit = UNITS * block
    units = groups // UNITS
    per = UNITS * SLOTS

    stage = lax.axis_index("pipe")
    e_idx = lax.axis_index("exp")
    y = lax.axis_index("pair")
    me = e_idx * ys + y
    cx = lax.div(e_idx, SIDE)
    cz = lax.rem(e_idx, SIDE)

    def ring(d):
        return min(d, SIDE - d)

    offsets = [
        (dx, dz, dy)
        for dx in range(zs // SIDE)
        for dz in range(SIDE)
        for dy in range(ys)
        if dx or dz or dy
    ]
    offsets.sort(key=lambda o: -(ring(o[0]) + ring(o[1]) + o[2]))

    def peer(offset):
        dx, dz, dy = offset
        px = lax.rem(cx + dx, zs // SIDE)
        pz = lax.rem(cz + dz, SIDE)
        return px * SIDE + pz, lax.rem(y + dy, ys)

    loads = []
    for j in range(locals_):
        pieces = []
        for k, (source, target) in enumerate(
            ((wgate_ref, wg), (wup_ref, wu), (wdown_ref, wd))
        ):
            tall = target.shape[1] // CUTS
            for cut in range(CUTS):
                part = pl.ds(cut * tall, tall)
                sem = w_sem.at[(3 * j + k) * CUTS + cut]
                pieces.append(
                    pltpu.make_async_copy(source.at[0, j, part], target.at[j, part], sem)
                )
        loads.append(pieces)

    def from_input(m):
        return pltpu.make_async_copy(hidden_ref.at[m], hbuf.at[m], h_sem.at[m])

    small = (
        pltpu.make_async_copy(routes_hbm, routes_ref, i_sem.at[0]),
        pltpu.make_async_copy(probs_hbm, probs_ref, i_sem.at[1]),
        pltpu.make_async_copy(gain_hbm, gain_ref, i_sem.at[2]),
    )
    for load in small:
        load.start()

    @pl.when(stage == 0)
    def _():
        for m in range(micro):
            from_input(m).start()

    for j in range(locals_):
        for load in loads[j]:
            load.start()

    barrier = pltpu.get_barrier_semaphore()
    for offset in offsets:
        pe, py = peer(offset)
        pl.semaphore_signal(barrier, inc=1, device_id={"exp": pe, "pair": py}, device_id_type=MESH)

    @pl.when(stage > 0)
    def _():
        pl.semaphore_signal(barrier, inc=1, device_id={"pipe": stage - 1}, device_id_type=MESH)

    @pl.when(stage < stages - 1)
    def _():
        pl.semaphore_signal(barrier, inc=1, device_id={"pipe": stage + 1}, device_id_type=MESH)

    def row_parts(index):
        d = fdiv(index, block)
        r = index - block * d
        q = fdiv(r, SLOTS)
        return d, q, r - SLOTS * q

    down, _, _ = row_parts(iota((unit, 1), 0))
    lane = iota((unit, LANES), 1)
    base = lane - locals_ * down
    for j in range(locals_):
        for u in range(units):
            first = locals_ * u * UNITS + j
            sel[j, pl.ds(u * unit, unit)] = jnp.where(base == first, 1.0, 0.0).astype(BF16)
    _, q, s = row_parts(iota((unit, 1), 0))
    pick_g[...] = jnp.where(fdiv(iota((1, STRIPS * rows), 1), rows) == q, s + 1.0, -1.0)


    def part_of(at):
        return pl.ds(pl.multiple_of(at * block, block), block)

    def out_copy_of(m, c, at, pe, py):
        return pltpu.make_async_remote_copy(
            src_ref=sendbuf.at[m, c, part_of(at)],
            dst_ref=recvbuf.at[m, c, part_of(me)],
            send_sem=a_sem.at[m, c, at],
            recv_sem=ar_sem.at[m, c, me],
            device_id={"exp": pe, "pair": py},
            device_id_type=MESH,
        )

    def in_copy_of(m, c, at, pe, py):
        return pltpu.make_async_remote_copy(
            src_ref=sendbuf.at[m, c, part_of(at)],
            dst_ref=recvbuf.at[m, c, part_of(at)],
            send_sem=a_sem.at[m, c, at],
            recv_sem=ar_sem.at[m, c, at],
            device_id={"exp": pe, "pair": py},
            device_id_type=MESH,
        )

    def back_copy_of(m, c, at, pe, py):
        return pltpu.make_async_remote_copy(
            src_ref=backbuf.at[m, c, part_of(at)],
            dst_ref=homebuf.at[m, c, part_of(me)],
            send_sem=b_sem.at[m, c, at],
            recv_sem=br_sem.at[m, c, me],
            device_id={"exp": pe, "pair": py},
            device_id_type=MESH,
        )

    def home_copy_of(m, c, at, pe, py):
        return pltpu.make_async_remote_copy(
            src_ref=backbuf.at[m, c, part_of(at)],
            dst_ref=homebuf.at[m, c, part_of(at)],
            send_sem=b_sem.at[m, c, at],
            recv_sem=br_sem.at[m, c, at],
            device_id={"exp": pe, "pair": py},
            device_id_type=MESH,
        )

    def hand_copy(m):
        return pltpu.make_async_remote_copy(
            src_ref=obuf.at[m],
            dst_ref=hbuf.at[m],
            send_sem=hs_sem.at[m],
            recv_sem=h_sem.at[m],
            device_id={"pipe": stage + 1},
            device_id_type=MESH,
        )

    def out_copy(m):
        return pltpu.make_async_copy(obuf.at[m], out_ref.at[0, m], o_sem.at[m])

    same = (iota((rows, rows), 0) == iota((rows, rows), 1)).astype(F32).astype(BF16)
    earlier = (iota((rows, rows), 0) >= iota((rows, rows), 1)).astype(F32).astype(BF16)

    def out_sent(m, j):
        for offset in offsets:
            pe, py = peer(offset)
            out_copy_of(m, j, pe * ys + py, pe, py).wait_send()

    def back_sent(m, j):
        for offset in offsets:
            pe, py = peer(offset)
            back_copy_of(m, j, pe * ys + py, pe, py).wait_send()

    last = locals_ - 1

    def settle():
        _, q, s = row_parts(iota((1, unit), 1))
        pick_s[...] = jnp.where(fdiv(iota((STRIPS * rows, 1), 0), rows) == q, s + 1.0, -1.0)
        d, q, s = row_parts(iota((1, unit), 1))
        moved_to = q * per + d * SLOTS + s
        unpack[...] = jnp.where(iota((unit, unit), 0) == moved_to, 1.0, 0.0).astype(BF16)
        d, q, s = row_parts(iota((unit, 1), 0))
        moved_to = q * per + d * SLOTS + s
        repack[...] = jnp.where(iota((unit, unit), 1) == moved_to, 1.0, 0.0).astype(BF16)

    def route(m):
        probs = probs_ref[0, m]
        normal = dot_nt(same, (probs / jnp.sum(probs, axis=0, keepdims=True)).astype(BF16))
        chosen = dot_nt(same, routes_ref[0, m].astype(F32).astype(BF16))
        lane = iota((rows, LANES), 1)
        mask = jnp.zeros((rows, LANES), F32)
        weight = jnp.zeros((rows, LANES), F32)
        for k in range(chosen.shape[1]):
            hit = lane == chosen[:, k : k + 1]
            mask = mask + jnp.where(hit, 1.0, 0.0)
            weight = weight + jnp.where(hit, normal[:, k : k + 1], 0.0)
        ranks = (mask * dot(earlier, mask.astype(BF16))).astype(BF16)
        code[0] = jnp.concatenate([ranks] * STRIPS, axis=0)
        code[1] = jnp.concatenate([weight.astype(BF16)] * STRIPS, axis=0)
        gather(0)

    def gather(j):
        for u in range(units):
            here = pl.ds(u * unit, unit)
            found = dot_nt(sel[j, here], code[0]) == pick_g[...]
            gath[j, here] = jnp.where(found, 1.0, 0.0).astype(BF16)

    def weigh(m):
        for j in range(locals_):
            for u in range(units):
                here = pl.ds(u * unit, unit)
                there = slice(u * unit, (u + 1) * unit)
                hits = dot_nt(code[0], sel[j, here]) == pick_s[...]
                shares = jnp.where(hits, dot_nt(code[1], sel[j, here]), 0.0)
                comb[lax.rem(m, 2), j, :, there] = shares.astype(BF16)

    def prepare(m):
        from_input(m).wait()
        state = hbuf[m].astype(F32)
        scale = lax.rsqrt(jnp.mean(state * state, axis=-1, keepdims=True) + EPS)
        normed = (state * scale * gain_ref[...]).astype(BF16)
        for q in range(STRIPS):
            xq[q * rows : (q + 1) * rows] = normed[:, q * qw : (q + 1) * qw]

    def dispatch(m, j):
        for u in range(units):
            here = pl.ds(u * unit, unit)
            sendbuf[m, j, here] = dot(gath[j, here], xq[...]).astype(BF16)
        recvbuf[m, j, part_of(me)] = sendbuf[m, j, part_of(me)]
        if j > 0:
            if ORDERED[1]:
                out_sent(m, j - 1)
        elif ORDERED[0]:

            @pl.when(m > 0)
            def _():
                back_sent(m - 1, last)

        for offset in offsets:
            pe, py = peer(offset)
            out_copy_of(m, j, pe * ys + py, pe, py).start()

    def expert(m, j):
        for offset in reversed(offsets):
            pe, py = peer(offset)
            in_copy_of(m, j, pe * ys + py, pe, py).wait_recv()
        for u in range(units):
            apart = dot(unpack[...], recvbuf[m, j, u * unit : (u + 1) * unit]).astype(BF16)
            for q in range(STRIPS):
                xe[u * per : (u + 1) * per, q * qw : (q + 1) * qw] = apart[q * per : (q + 1) * per]

        @pl.when(m == 0)
        def _():
            for load in loads[j]:
                load.wait()

        held = xe[...]
        for f in range(0, ff, 256):
            cols = slice(f, f + 256)
            gate = dot(held, wg[j, :, cols])
            upward = dot(held, wu[j, :, cols])
            hid[:, cols] = (jax.nn.silu(gate) * upward).astype(BF16)
        for q in range(STRIPS):
            made = dot(hid[...], wd[j, :, q * qw : (q + 1) * qw]).astype(BF16)
            for u in range(units):
                stack[u, q * per : (q + 1) * per] = made[u * per : (u + 1) * per]
        for u in range(units):
            backbuf[m, j, u * unit : (u + 1) * unit] = dot(repack[...], stack[u]).astype(BF16)
        homebuf[m, j, part_of(me)] = backbuf[m, j, part_of(me)]
        if j > 0:
            if ORDERED[3]:
                back_sent(m, j - 1)
        elif ORDERED[2]:
            out_sent(m, last)
        for offset in offsets:
            pe, py = peer(offset)
            back_copy_of(m, j, pe * ys + py, pe, py).start()

    def finish(m):
        mixed = jnp.zeros((STRIPS * rows, qw), F32)
        for j in range(locals_):
            for offset in reversed(offsets):
                pe, py = peer(offset)
                home_copy_of(m, j, pe * ys + py, pe, py).wait_recv()
            mixed = mixed + dot(comb[lax.rem(m, 2), j], homebuf[m, j])
        for q in range(STRIPS):
            cols = slice(q * qw, (q + 1) * qw)
            added = hbuf[m, :, cols].astype(F32) + mixed[q * rows : (q + 1) * rows]
            obuf[m, :, cols] = added.astype(BF16)

        @pl.when(stage < stages - 1)
        def _():
            hand_copy(m).start()

        out_copy(m).start()

    for load in small:
        load.wait()
    route(0)
    linked = (stage > 0).astype(jnp.int32) + (stage < stages - 1).astype(jnp.int32)
    pl.semaphore_wait(barrier, len(offsets) + linked)

    @pl.loop(0, micro + 1)
    def _(i):
        def finish_at(place):
            now = i == micro if place == 0 else i < 0
            for at in range(stages):
                for step in range(micro - 1):
                    if PLACES[at][step] == place:
                        now = jnp.logical_or(now, jnp.logical_and(stage == at, i == step + 1))

            @pl.when(now)
            def _():
                finish(i - 1)

        finish_at(0)

        @pl.when(i < micro)
        def _():
            prepare(i)

        finish_at(1)

        @pl.when(i < micro)
        def _():
            dispatch(i, 0)

        finish_at(2)

        @pl.when(i < micro)
        def _():
            for j in range(1, locals_):

                @pl.when(i == 0)
                def _():
                    gather(j)

                dispatch(i, j)

        finish_at(3)

        @pl.when(i < micro)
        def _():
            pl.when(i == 0)(settle)
            weigh(i)
            for j in range(locals_):
                expert(i, j)

        @pl.when(i < micro - 1)
        def _():
            route(i + 1)
            for j in range(1, locals_):
                gather(j)

    if ORDERED[0]:
        back_sent(micro - 1, last)

    @pl.loop(0, micro)
    def _(m):
        if not ORDERED[0]:
            back_sent(m, last)
        if not ORDERED[1]:
            for j in range(last):
                out_sent(m, j)
        if not ORDERED[2]:
            out_sent(m, last)
        if not ORDERED[3]:
            for j in range(last):
                back_sent(m, j)

        @pl.when(stage < stages - 1)
        def _():
            hand_copy(m).wait_send()

        out_copy(m).wait()


def relayed(hidden_in, routes, gate_probs, norm_gain, w_gate, w_up, w_down):
    routes = jnp.swapaxes(routes, 2, 3)
    gate_probs = jnp.swapaxes(gate_probs, 2, 3)
    micro, rows, width = hidden_in.shape
    _, locals_, _, ff = w_gate.shape
    stages, zs, ys = (lax.axis_size(a) for a in ("pipe", "exp", "pair"))
    groups = zs * ys
    block = STRIPS * SLOTS
    total = groups * block
    unit = UNITS * block
    qw = width // STRIPS
    spread = STRIPS * rows
    dma = pltpu.SemaphoreType.DMA
    anywhere = pl.BlockSpec(memory_space=pl.ANY)
    moved = pltpu.VMEM((micro, locals_, total, qw), BF16)
    return pl.pallas_call(
        functools.partial(relay_kernel, stages, zs, ys),
        out_shape=jax.ShapeDtypeStruct((1, micro, rows, width), BF16),
        in_specs=[anywhere] * 7,
        out_specs=anywhere,
        scratch_shapes=[
            pltpu.VMEM(routes.shape, jnp.int32),
            pltpu.VMEM(gate_probs.shape, F32),
            pltpu.VMEM(norm_gain.shape, F32),
            pltpu.VMEM((locals_, width, ff), BF16),
            pltpu.VMEM((locals_, width, ff), BF16),
            pltpu.VMEM((locals_, ff, width), BF16),
            pltpu.VMEM((micro, rows, width), BF16),
            pltpu.VMEM((micro, rows, width), BF16),
            pltpu.VMEM((spread, qw), BF16),
            moved,
            moved,
            moved,
            moved,
            pltpu.VMEM((groups * SLOTS, width), BF16),
            pltpu.VMEM((groups * SLOTS, ff), BF16),
            pltpu.VMEM((groups // UNITS, unit, qw), BF16),
            pltpu.VMEM((locals_, total, LANES), BF16),
            pltpu.VMEM((unit, spread), F32),
            pltpu.VMEM((spread, unit), F32),
            pltpu.VMEM((2, spread, LANES), BF16),
            pltpu.VMEM((locals_, total, spread), BF16),
            pltpu.VMEM((2, locals_, spread, total), BF16),
            pltpu.VMEM((unit, unit), BF16),
            pltpu.VMEM((unit, unit), BF16),
            dma((3,)),
            dma((3 * locals_ * CUTS,)),
            dma((micro,)),
            dma((micro,)),
            dma((micro,)),
            dma((micro, locals_, groups)),
            dma((micro, locals_, groups)),
            dma((micro, locals_, groups)),
            dma((micro, locals_, groups)),
        ],
        compiler_params=pltpu.CompilerParams(
            collective_id=0, has_side_effects=True, vmem_limit_bytes=VMEM_LIMIT
        ),
    )(hidden_in, routes, gate_probs, norm_gain, w_gate, w_up, w_down)


def solution(mesh):
    in_specs = (
        P(None, ("exp", "pair"), None),
        P("pipe", None, ("exp", "pair"), None),
        P("pipe", None, ("exp", "pair"), None),
        P("pipe", None),
        P("pipe", ("exp", "pair"), None, None),
        P("pipe", ("exp", "pair"), None, None),
        P("pipe", ("exp", "pair"), None, None),
    )
    out_specs = P("pipe", None, ("exp", "pair"), None)
    return jax.shard_map(
        relayed, mesh=mesh, in_specs=in_specs, out_specs=out_specs, check_vma=False
    )
```
